128 devices in a mesh: grp: 4 (over x, y), gx: 32 (over z, core).
Axes of the slice: x: 2, y: 2, z: 16, core: 2. Of those that a mesh axis runs over, the one named last changes fastest.
The devices are a block of a 8x8x16 slice.
Arguments:
- wave_now: float32 [12, 512, 64, 256], P('grp', 'gx'), parts along dimension 0
- wave_prev: float32 [12, 512, 64, 256], P('grp', 'gx'), parts along dimension 0
- velocity: float32 [2048, 64, 256], P(('grp', 'gx')), parts along dimension 0, may hold values from 0.05 to 0.18
- snapshots: float32 [12, 2, 512, 64, 256], P('grp', None, 'gx'), parts along dimension 0, may hold values from -6 to 6
- traces: float32 [16, 1024], P('grp'), parts along dimension 0, may hold values from -18 to 18
- recv_x: int32 [4096], P('grp'), parts along dimension 0, may hold values from 0 to 511
- recv_y: int32 [4096], P('grp'), parts along dimension 0, may hold values from 0 to 63
- recv_z: int32 [4096], P('grp'), parts along dimension 0, may hold values from 0 to 255
- recv_shot: int32 [4096], P('grp'), parts along dimension 0, may hold values from 0 to 2
- snap_step: int32 [16, 3], P('grp'), parts along dimension 0, may hold values from 0 to 1
Outputs:
- image: float32 [2048, 64, 256], P(('grp', 'gx')), parts along dimension 0
- final_now: float32 [12, 512, 64, 256], P('grp', 'gx'), parts along dimension 0
- final_prev: float32 [12, 512, 64, 256], P('grp', 'gx'), parts along dimension 0
- energies: float32 [16, 3], P('grp'), parts along dimension 0
The draws below stay inside these ranges and needn't reach their ends.
There are 4 independent parts, one for each index of `grp`. The reference program is written for one: setup_inputs(seed, part) draws one part's arguments, and reference() takes and returns one part's arrays. A program takes and returns all parts, laid end to end along the dimension named above; each array names one. Nothing has to cross between parts.
All inputs are finite; a program needn't handle non-finite values.
Results may differ from the reference program's by a relative error of at most 0.00021.
Values sent between devices are 32-bit elements; how exact they have to be, the bound alone decides.
A program may use at most 128 MiB of HBM per device.

```python
import jax
import jax.numpy as jnp
from jax import lax

NY = 64
NZ = 256
RECV = 1024
SHOTS = 3
STEPS = 4
SNAPS = 2
NX = 512
CELLS = 8388608


def field_scale(key):
    position = jnp.arange(NX).astype(jnp.float32) / (NX - 1)
    row_scale = 10.0 ** jax.random.uniform(jax.random.fold_in(key, 21), (NX,), jnp.float32, -0.5, 0.5)
    column_scale = 10.0 ** jax.random.uniform(jax.random.fold_in(key, 22), (NY,), jnp.float32, -0.5, 0.5)
    trend = 1.0 + 2.0 * position
    scale = (row_scale * trend)[:, None] * column_scale[None, :]
    return scale[None, :, :, None] * 0.5


def now_field(key):
    base = jax.random.normal(jax.random.fold_in(key, 20), (SHOTS, NX, NY, NZ), jnp.float32)
    return base * field_scale(key)


def speed_field(key):
    return jax.random.uniform(jax.random.fold_in(key, 30), (NX, NY, NZ), jnp.float32, 0.05, 0.18)


def draw_wave_now(key, part):
    return now_field(key).astype(jnp.float32)


def draw_velocity(key, part):
    return speed_field(key).astype(jnp.float32)


def draw_wave_prev(key, part):
    result = jnp.clip(jax.random.normal(jax.random.fold_in(key, 40), (SHOTS, NX, NY, NZ), jnp.float32), -6.0, 6.0)
    return result.astype(jnp.float32)


def plant(entries, key, least, largest):
    extent = entries.shape
    spot = [jax.random.randint(jax.random.fold_in(key, axis), (), 0, extent[axis]) for axis in range(len(extent))]
    entries = entries.at[tuple(spot)].set(least)
    longest = extent.index(max(extent))
    spot[longest] = (spot[longest] + 1) % extent[longest]
    return entries.at[tuple(spot)].set(largest)


def levels(key, extent, cuts, least, top_value):
    factor_of, own = 1.0, jax.random.fold_in(key, 6)
    for dim, shards_of in cuts:
        heights = jnp.exp(jax.random.uniform(jax.random.fold_in(own, dim), (shards_of,), jnp.float32, least / len(cuts), top_value / len(cuts)))
        factor_of = factor_of * jnp.repeat(heights, extent[dim] // shards_of).reshape([-1 if axis == dim else 1 for axis in range(len(extent))])
    return factor_of


def gaussian(own_key, extent, spread, most, shards=(), dtype=jnp.bfloat16):
    array = jax.random.normal(own_key, extent, jnp.float32) * spread
    if len(shards) > 0:
        array = levels(own_key, extent, shards, -0.22, 0.18) * array
    return jnp.clip(array, min=-most, max=most).astype(dtype)


def setup_inputs(seed: int = 0, part: int = 0) -> dict:
    key_list = jax.random.split(jax.random.key(seed), 11)
    part_keys = jax.random.split(jax.random.fold_in(key_list[10], part), 11)
    wave_now = draw_wave_now(jax.random.fold_in(jax.random.fold_in(key_list[10], part), 71), part)
    wave_prev = draw_wave_prev(jax.random.fold_in(jax.random.fold_in(key_list[10], part), 71), part)
    velocity = draw_velocity(jax.random.fold_in(jax.random.fold_in(key_list[10], part), 71), part)
    snapshots = gaussian(part_keys[3], (SHOTS, SNAPS, NX, NY, NZ), 1.0, 6.0, ((2, 32),), jnp.float32)
    traces = gaussian(part_keys[4], (STEPS, RECV), 3.0, 18.0, (), jnp.float32)
    recv_x = plant(jax.random.randint(part_keys[5], (RECV,), 0, NX), jax.random.fold_in(part_keys[5], 1), 0, NX - 1).astype(jnp.int32)
    recv_y = plant(jax.random.randint(part_keys[6], (RECV,), 0, NY), jax.random.fold_in(part_keys[6], 1), 0, NY - 1).astype(jnp.int32)
    recv_z = plant(jax.random.randint(part_keys[7], (RECV,), 0, NZ), jax.random.fold_in(part_keys[7], 1), 0, NZ - 1).astype(jnp.int32)
    recv_shot = plant(jax.random.randint(part_keys[8], (RECV,), 0, SHOTS), jax.random.fold_in(part_keys[8], 1), 0, SHOTS - 1).astype(jnp.int32)
    snap_step = plant(jax.random.randint(part_keys[9], (STEPS, SHOTS), 0, SNAPS), jax.random.fold_in(part_keys[9], 1), 0, SNAPS - 1).astype(jnp.int32)
    return dict(wave_now=wave_now, wave_prev=wave_prev, velocity=velocity, snapshots=snapshots, traces=traces, recv_x=recv_x, recv_y=recv_y, recv_z=recv_z, recv_shot=recv_shot, snap_step=snap_step)


COEFS = (-205.0 / 72.0, 8.0 / 5.0, -1.0 / 5.0, 8.0 / 315.0, -1.0 / 560.0)

def laplace(field):
    length, depth_y, depth_z = (field.shape[1], field.shape[2], field.shape[3])
    padded = jnp.pad(field, ((0, 0), (4, 4), (4, 4), (4, 4)))

    def cut(shift_x, shift_y, shift_z):
        return padded[:, 4 + shift_x:4 + shift_x + length, 4 + shift_y:4 + shift_y + depth_y, 4 + shift_z:4 + shift_z + depth_z]
    total = 3.0 * COEFS[0] * cut(0, 0, 0)
    for reach in range(1, 5):
        total = total + COEFS[reach] * (cut(reach, 0, 0) + cut(-reach, 0, 0) + cut(0, reach, 0) + cut(0, -reach, 0) + cut(0, 0, reach) + cut(0, 0, -reach))
    return total

def reference(wave_now, wave_prev, velocity, snapshots, traces, recv_x, recv_y, recv_z, recv_shot, snap_step):
    current, previous = (wave_now, wave_prev)
    image = jnp.zeros(velocity.shape, jnp.float32)
    shot_ids = jnp.arange(SHOTS).astype(jnp.int32)
    totals = []
    for step in range(STEPS):
        fresh = 2.0 * current - previous + velocity[None] * laplace(current)
        source = traces[step] * velocity[recv_x, recv_y, recv_z]
        fresh = fresh.at[recv_shot, recv_x, recv_y, recv_z].add(source)
        energy = lax.optimization_barrier(jnp.sum(fresh * fresh, axis=(1, 2, 3)))
        totals.append(energy)
        weight = 1.0 / jnp.sqrt(energy / CELLS + 1e-06)
        chosen = snapshots[shot_ids, snap_step[step].astype(jnp.int32)]
        image = image + lax.optimization_barrier(jnp.sum(weight[:, None, None, None] * chosen * fresh, axis=0))
        previous, current = (current, fresh)
    return (image, current, previous, jnp.stack(totals))
```

```python
import functools

import jax
import jax.numpy as jnp
from jax import lax
from jax.experimental import pallas as pl
from jax.experimental.pallas import tpu as pltpu
from jax.sharding import PartitionSpec as P

MESH = pl.DeviceIdType.MESH
SCALE = 5040.0
CENTRE = -43050.0
REACH = (0.0, 8064.0, -1008.0, 128.0, -9.0)
HALO = 4
ROWS = 4
F32 = jnp.float32
BF16 = jnp.bfloat16


def band(size, period):
    row = lax.broadcasted_iota(jnp.int32, (size, size), 0)
    col = lax.broadcasted_iota(jnp.int32, (size, size), 1)
    gap = jnp.abs(row - col)
    same = (row // period) == (col // period)
    value = jnp.zeros((size, size), F32)
    for k in range(1, HALO + 1):
        value = jnp.where((gap == k) & same, REACH[k], value)
    return value.astype(BF16)


def dot(a, b, dims=((1,), (0,))):
    return lax.dot_general(a, b, (dims, ((), ())), preferred_element_type=F32)


def kernel(
    n,
    now_hbm,
    prev_hbm,
    vel_hbm,
    snap_hbm,
    traces,
    recv_x,
    recv_y,
    recv_z,
    recv_shot,
    snap_step,
    image_hbm,
    last_hbm,
    before_hbm,
    energy_out,
    w,
    vel,
    snap,
    corr,
    onehot,
    amps,
    band_y,
    band_z,
    squares,
    image,
    row_mine,
    row_partner,
    row_chip,
    rows_all,
    load_edge,
    load_mid,
    load_prev,
    load_vel,
    load_snap,
    send_sem,
    recv_sem,
    ready_sem,
    pair_send,
    pair_recv,
    all_send,
    all_recv,
    out_last,
    out_before,
    out_image,
):
    shots, slab, ny, nz = now_hbm.shape
    steps, count = traces.shape
    blocks = slab // ROWS
    low, high = HALO, HALO + slab
    me = lax.axis_index("gx")
    right, left = lax.rem(me + 1, n), lax.rem(me + n - 1, n)

    barrier = pltpu.get_barrier_semaphore()
    for other in (left, right):
        pl.semaphore_signal(barrier, inc=1, device_id={"gx": other}, device_id_type=MESH)

    def edge_load(s, side):
        at = 0 if side == 0 else slab - HALO
        return pltpu.make_async_copy(
            now_hbm.at[s, pl.ds(at, HALO)], w.at[0, s, pl.ds(low + at, HALO)], load_edge.at[side, s]
        )

    def mid_load(s):
        return pltpu.make_async_copy(
            now_hbm.at[s, pl.ds(HALO, slab - 2 * HALO)],
            w.at[0, s, pl.ds(low + HALO, slab - 2 * HALO)],
            load_mid.at[s],
        )

    def prev_load(s):
        return pltpu.make_async_copy(prev_hbm.at[s], w.at[1, s, pl.ds(low, slab)], load_prev.at[s])

    def snap_load(s):
        return pltpu.make_async_copy(snap_hbm.at[s], snap.at[s], load_snap.at[s])

    vel_load = pltpu.make_async_copy(vel_hbm, vel, load_vel)

    for s in range(shots):
        for side in range(2):
            edge_load(s, side).start()
    vel_load.start()
    for s in range(shots):
        mid_load(s).start()
        prev_load(s).start()
    for s in range(shots):
        snap_load(s).start()

    def halo_copy(t, s, side):
        parity = lax.rem(t, 2)
        if side == 0:
            source, target, device = low, high, left
        else:
            source, target, device = high - HALO, 0, right
        return pltpu.make_async_remote_copy(
            src_ref=w.at[parity, s, pl.ds(source, HALO)],
            dst_ref=w.at[parity, s, pl.ds(target, HALO)],
            send_sem=send_sem.at[side, t, s],
            recv_sem=recv_sem.at[side, t, s],
            device_id={"gx": device},
            device_id_type=MESH,
        )

    has = (me > 0, me < n - 1)

    pl.semaphore_wait(barrier, 2)
    for s in range(shots):
        for side in range(2):
            edge_load(s, side).wait()

            @pl.when(has[side])
            def _():
                halo_copy(0, s, side).start()

    zeros = jnp.zeros((HALO, ny, nz), F32)
    for side, at in ((0, 0), (1, high)):

        @pl.when(jnp.logical_not(has[side]))
        def _():
            for parity in range(2):
                for s in range(shots):
                    w[parity, s, pl.ds(at, HALO)] = zeros

    band_y[...] = band(ROWS * ny, ny)
    band_z[...] = band(nz, nz)
    local = recv_x[...] - me * slab
    inside = (local >= 0) & (local < slab)
    place = jnp.where(inside, (recv_shot[...] * slab + local) * ny + recv_y[...], -1)

    def fill_onehot(b, carry):
        index = lax.broadcasted_iota(jnp.int32, (ROWS * ny, count), 0) + b * (ROWS * ny)
        onehot[b] = jnp.where(index == place, 1.0, 0.0).astype(BF16)
        return carry

    lax.fori_loop(0, shots * blocks, fill_onehot, 0)
    along = lax.broadcasted_iota(jnp.int32, (nz, count), 0) == recv_z[...]
    for t in range(steps):
        amp = traces[t : t + 1, :] * SCALE
        top = amp.astype(BF16).astype(F32)
        amps[t, 0] = jnp.where(along, top, 0.0).astype(BF16)
        amps[t, 1] = jnp.where(along, amp - top, 0.0).astype(BF16)

    vel_load.wait()
    vel[...] = vel[...] * (1.0 / SCALE)

    def fold(value):
        return jnp.sum(value.reshape(ny // 8, 8, nz), axis=0)

    def record(t, s, x, fresh):
        chosen = snap[s, snap_step[t, s], x]
        corr[t, s, x] = chosen * fresh
        return fold(fresh * fresh)

    def block_stage(t, s):
        cur = lax.rem(t, 2)
        nxt = 1 - cur
        for b in range(blocks):
            inner = 0 < b < blocks - 1
            x0 = b * ROWS
            v = w[cur, s, pl.ds(low + x0, ROWS)].reshape(ROWS * ny, nz)
            top = v.astype(BF16)
            rest = (v - top.astype(F32)).astype(BF16)
            acc = dot(top, band_z[...]) + dot(rest, band_z[...])
            acc = acc + dot(band_y[...], top) + dot(band_y[...], rest)
            hot = onehot[s * blocks + b]
            acc = acc + dot(hot, amps[t, 0], ((1,), (1,))) + dot(hot, amps[t, 1], ((1,), (1,)))
            acc = acc.reshape(ROWS, ny, nz)
            total = jnp.zeros((8, nz), F32)
            for i in range(ROWS):
                x = x0 + i
                centre = w[cur, s, low + x]
                value = acc[i] + CENTRE * centre
                for k in range(1, HALO + 1):
                    near = []
                    if x + k < slab:
                        near.append(w[cur, s, low + x + k])
                    if x - k >= 0:
                        near.append(w[cur, s, low + x - k])
                    pair = near[0] + near[1] if len(near) == 2 else near[0]
                    value = value + REACH[k] * pair
                fresh = 2.0 * centre - w[nxt, s, low + x] + vel[x] * value
                w[nxt, s, low + x] = fresh
                if inner:
                    total = total + record(t, s, x, fresh)
            if inner:
                if b == 1:
                    squares[t, s] = total
                else:
                    squares[t, s] = squares[t, s] + total

    def edge_stage(t, s):
        cur = lax.rem(t, 2)
        nxt = 1 - cur
        for side in range(2):

            @pl.when(has[side])
            def _():
                halo_copy(t, s, 1 - side).wait_recv()

            for i in range(HALO):
                x = i if side == 0 else slab - 1 - i
                sign = -1 if side == 0 else 1
                add = None
                for k in range(i + 1, HALO + 1):
                    term = REACH[k] * w[cur, s, low + x + sign * k]
                    add = term if add is None else add + term
                w[nxt, s, low + x] = w[nxt, s, low + x] + vel[x] * add

            @pl.when(has[side] & (t < steps - 1))
            def _():
                halo_copy(t + 1, s, side).start()

        for side in range(2):

            @pl.when(has[side])
            def _():
                halo_copy(t, s, side).wait_send()

        total = squares[t, s]
        for i in range(HALO):
            for x in (i, slab - 1 - i):
                total = total + record(t, s, x, w[nxt, s, low + x])
        squares[t, s] = total

        @pl.when(t == steps - 2)
        def _():
            before_copy(s).start()

        @pl.when(t == steps - 1)
        def _():
            last_copy(s).start()

    def before_copy(s):
        return pltpu.make_async_copy(
            w.at[(steps - 1) % 2, s, pl.ds(low, slab)], before_hbm.at[s], out_before.at[s]
        )

    def last_copy(s):
        return pltpu.make_async_copy(
            w.at[steps % 2, s, pl.ds(low, slab)], last_hbm.at[s], out_last.at[s]
        )

    rounds = 0
    while 2 ** (rounds + 1) < n // 2:
        rounds += 1
    rounds += 1

    def meet(m):
        for j in range(rounds + 1):

            @pl.when(m == shots + 1 + j)
            def _():
                if j > 0:
                    pl.semaphore_wait(ready_sem.at[j - 1], 2)
                if j < rounds:
                    for other in (lax.rem(me + 2**j, n), lax.rem(me + n - 2**j, n)):
                        pl.semaphore_signal(
                            ready_sem.at[j], inc=1, device_id={"gx": other}, device_id_type=MESH
                        )

    def turn(m, carry):
        s = lax.rem(m, shots)
        t = m // shots

        @pl.when(t > 0)
        def _():
            edge_stage(t - 1, s)

        @pl.when(t == 0)
        def _():
            mid_load(s).wait()
            prev_load(s).wait()

            @pl.when(s == 0)
            def _():
                for other in range(shots):
                    snap_load(other).wait()

        @pl.when(t < steps)
        def _():
            block_stage(t, s)

        meet(m)
        return carry

    lax.fori_loop(0, shots * (steps + 1), turn, 0)

    lane = lax.broadcasted_iota(jnp.int32, (1, 128), 1)
    mine = jnp.zeros((1, 128), F32)
    for t in range(steps):
        for s in range(shots):
            amount = jnp.sum(jnp.sum(squares[t, s], axis=0, keepdims=True), axis=1, keepdims=True)
            mine = jnp.where(lane == t * shots + s, amount, mine)
    row_mine[...] = mine
    partner = me + 1 - 2 * lax.rem(me, 2)
    pair = pltpu.make_async_remote_copy(
        src_ref=row_mine,
        dst_ref=row_partner,
        send_sem=pair_send,
        recv_sem=pair_recv,
        device_id={"gx": partner},
        device_id_type=MESH,
    )
    pair.start()
    pair.wait()
    chips = n // 2
    chip = me // 2
    both = mine + row_partner[...]
    row_chip[...] = both
    rows_all[chip] = both

    def share(k):
        return pltpu.make_async_remote_copy(
            src_ref=row_chip,
            dst_ref=rows_all.at[chip],
            send_sem=all_send,
            recv_sem=all_recv,
            device_id={"gx": lax.rem(me + 2 * k, n)},
            device_id_type=MESH,
        )

    for k in range(1, chips):
        share(k).start()
    everyone = pltpu.make_async_remote_copy(
        src_ref=rows_all.at[pl.ds(0, chips - 1)],
        dst_ref=rows_all.at[pl.ds(0, chips - 1)],
        send_sem=all_send,
        recv_sem=all_recv,
        device_id={"gx": right},
        device_id_type=MESH,
    )
    everyone.wait()
    energy = jnp.sum(rows_all[...], axis=0)
    cells = float(slab * ny * nz) * n
    weight = 1.0 / jnp.sqrt(energy / cells + 1e-6)

    weights = [weight[:, i : i + 1] for i in range(steps * shots)]

    def paint(x, carry):
        total = jnp.zeros((ny, nz), F32)
        for t in range(steps):
            for s in range(shots):
                total = total + weights[t * shots + s] * corr[t, s, x]
        image[x] = total
        image_copy(x).start()
        return carry

    def image_copy(x):
        return pltpu.make_async_copy(image.at[x], image_hbm.at[x], out_image.at[x])

    lax.fori_loop(0, slab, paint, 0)
    for t in range(steps):
        energy_out[t : t + 1, :] = energy[:, t * shots : (t + 1) * shots]
    for s in range(shots):
        before_copy(s).wait()
        last_copy(s).wait()
    for x in range(slab):
        image_copy(x).wait()


def per_device(
    n, now, prev, velocity, snapshots, traces, recv_x, recv_y, recv_z, recv_shot, snap_step
):
    shots, slab, ny, nz = now.shape
    snaps = snapshots.shape[1]
    steps, count = traces.shape
    blocks = slab // ROWS
    full = slab + 2 * HALO
    any_space = pl.BlockSpec(memory_space=pl.ANY)
    vmem = pl.BlockSpec(memory_space=pltpu.VMEM)
    smem = pl.BlockSpec(memory_space=pltpu.SMEM)
    dma = pltpu.SemaphoreType.DMA
    shape = functools.partial(jax.ShapeDtypeStruct, dtype=F32)
    return pl.pallas_call(
        functools.partial(kernel, n),
        out_shape=(
            shape((slab, ny, nz)),
            shape((shots, slab, ny, nz)),
            shape((shots, slab, ny, nz)),
            shape((steps, shots)),
        ),
        in_specs=[any_space] * 4 + [vmem] * 5 + [smem],
        out_specs=(any_space, any_space, any_space, vmem),
        scratch_shapes=[
            pltpu.VMEM((2, shots, full, ny, nz), F32),
            pltpu.VMEM((slab, ny, nz), F32),
            pltpu.VMEM((shots, snaps, slab, ny, nz), F32),
            pltpu.VMEM((steps, shots, slab, ny, nz), F32),
            pltpu.VMEM((shots * blocks, ROWS * ny, count), BF16),
            pltpu.VMEM((steps, 2, nz, count), BF16),
            pltpu.VMEM((ROWS * ny, ROWS * ny), BF16),
            pltpu.VMEM((nz, nz), BF16),
            pltpu.VMEM((steps, shots, 8, nz), F32),
            pltpu.VMEM((slab, ny, nz), F32),
            pltpu.VMEM((1, 128), F32),
            pltpu.VMEM((1, 128), F32),
            pltpu.VMEM((1, 128), F32),
            pltpu.VMEM((n // 2, 1, 128), F32),
            dma((2, shots)),
            dma((shots,)),
            dma((shots,)),
            dma,
            dma((shots,)),
            dma((2, steps, shots)),
            dma((2, steps, shots)),
            pltpu.SemaphoreType.REGULAR((8,)),
            dma,
            dma,
            dma,
            dma,
            dma((shots,)),
            dma((shots,)),
            dma((slab,)),
        ],
        compiler_params=pltpu.CompilerParams(
            collective_id=0, has_side_effects=True, vmem_limit_bytes=60 * 1024 * 1024
        ),
        name="rtm",
    )(
        now,
        prev,
        velocity,
        snapshots,
        traces,
        recv_x.reshape(1, -1),
        recv_y.reshape(1, -1),
        recv_z.reshape(1, -1),
        recv_shot.reshape(1, -1),
        snap_step,
    )


def solution(mesh):
    placed = (
        P("grp", "gx", None, None),
        P("grp", "gx", None, None),
        P(("grp", "gx"), None, None),
        P("grp", None, "gx", None, None),
        P("grp", None),
        P("grp"),
        P("grp"),
        P("grp"),
        P("grp"),
        P("grp", None),
    )
    return jax.shard_map(
        functools.partial(per_device, mesh.shape["gx"]),
        mesh=mesh,
        in_specs=placed,
        out_specs=(
            P(("grp", "gx"), None, None),
            P("grp", "gx", None, None),
            P("grp", "gx", None, None),
            P("grp", None),
        ),
        check_vma=False,
    )
```

```python
import functools

import jax
import jax.numpy as jnp
from jax import lax
from jax.experimental import pallas as pl
from jax.experimental.pallas import tpu as pltpu
from jax.sharding import PartitionSpec as P

MESH = pl.DeviceIdType.MESH
SCALE = 5040.0
CENTRE = -43050.0
REACH = (0.0, 8064.0, -1008.0, 128.0, -9.0)
HALO = 4
FLIGHT = 64
VMEM_SOURCES = 63 * 2**20
VMEM_STEPS = 60 * 2**20
ROWS = 4
F32 = jnp.float32
BF16 = jnp.bfloat16


def band(size, period):
    row = lax.broadcasted_iota(jnp.int32, (size, size), 0)
    col = lax.broadcasted_iota(jnp.int32, (size, size), 1)
    gap = jnp.abs(row - col)
    same = (row // period) == (col // period)
    value = jnp.zeros((size, size), F32)
    for k in range(1, HALO + 1):
        value = jnp.where((gap == k) & same, REACH[k], value)
    return value.astype(BF16)


def dot(a, b, dims=((1,), (0,))):
    return lax.dot_general(a, b, (dims, ((), ())), preferred_element_type=F32)


def kernel(
    n,
    now_hbm,
    prev_hbm,
    vel_hbm,
    snap_hbm,
    sources_hbm,
    snap_step,
    image_hbm,
    last_hbm,
    before_hbm,
    energy_out,
    own,
    image,
    halo,
    vel,
    snap,
    sources,
    corr,
    band_y,
    band_z,
    squares,
    spread,
    row_mine,
    row_partner,
    row_chip,
    rows_all,
    load_edge,
    load_mid,
    load_prev,
    load_vel,
    load_snap,
    load_sources,
    send_sem,
    recv_sem,
    ready_sem,
    pair_send,
    pair_recv,
    all_send,
    all_recv,
    out_last,
    out_before,
    out_image,
):
    shots, slab, ny, nz = now_hbm.shape
    steps, snaps = sources_hbm.shape[0], snap_hbm.shape[1]
    blocks = slab // ROWS
    me = lax.axis_index("gx")
    right, left = lax.rem(me + 1, n), lax.rem(me + n - 1, n)

    barrier = pltpu.get_barrier_semaphore()
    for other in (left, right):
        pl.semaphore_signal(barrier, inc=1, device_id={"gx": other}, device_id_type=MESH)

    def edge_load(s, side):
        planes = pl.ds(0 if side == 0 else slab - HALO, HALO)
        return pltpu.make_async_copy(
            now_hbm.at[s, planes], own.at[0, s, planes], load_edge.at[side, s]
        )

    def mid_load(s):
        planes = pl.ds(HALO, slab - 2 * HALO)
        return pltpu.make_async_copy(now_hbm.at[s, planes], own.at[0, s, planes], load_mid.at[s])

    def prev_load(s):
        return pltpu.make_async_copy(prev_hbm.at[s], own.at[1, s], load_prev.at[s])

    def snap_load(s):
        return pltpu.make_async_copy(snap_hbm.at[s], snap.at[s], load_snap.at[s])

    def sources_load(t, s):
        return pltpu.make_async_copy(sources_hbm.at[t, s], sources.at[t, s], load_sources.at[t, s])

    vel_load = pltpu.make_async_copy(vel_hbm, vel, load_vel)

    for s in range(shots):
        for side in range(2):
            edge_load(s, side).start()
    vel_load.start()
    for s in range(shots):
        mid_load(s).start()
        prev_load(s).start()
        sources_load(0, s).start()
        snap_load(s).start()
    for t in range(1, steps):
        for s in range(shots):
            sources_load(t, s).start()

    def halo_copy(t, s, side):
        parity = lax.rem(t, 2)
        device = left if side == 0 else right
        return pltpu.make_async_remote_copy(
            src_ref=own.at[parity, s, pl.ds(0 if side == 0 else slab - HALO, HALO)],
            dst_ref=halo.at[parity, s, 1 - side],
            send_sem=send_sem.at[side, t, s],
            recv_sem=recv_sem.at[side, t, s],
            device_id={"gx": device},
            device_id_type=MESH,
        )

    has = (me > 0, me < n - 1)

    pl.semaphore_wait(barrier, 2)
    for s in range(shots):
        for side in range(2):
            edge_load(s, side).wait()

            @pl.when(has[side])
            def _():
                halo_copy(0, s, side).start()

    zeros = jnp.zeros((HALO, ny, nz), F32)
    for side in range(2):

        @pl.when(jnp.logical_not(has[side]))
        def _():
            for parity in range(2):
                for s in range(shots):
                    halo[parity, s, side] = zeros

    band_y[...] = band(ROWS * ny, ny)
    band_z[...] = band(nz, nz)
    vel_load.wait()
    vel[...] = vel[...] * (1.0 / SCALE)

    def fold(value):
        return jnp.sum(value.reshape(ny // 8, 8, nz), axis=0)

    def record(t, s, x, fresh):
        chosen = snap[s, 0, x]
        for k in range(1, snaps):
            chosen = jnp.where(snap_step[t, s] == k, snap[s, k, x], chosen)
        corr[t, s, x] = chosen * fresh
        return fold(fresh * fresh)

    def block_stage(t, s):
        cur = lax.rem(t, 2)
        nxt = 1 - cur
        for b in range(blocks):
            inner = 0 < b < blocks - 1
            x0 = b * ROWS
            v = own[cur, s, pl.ds(x0, ROWS)].reshape(ROWS * ny, nz)
            top = v.astype(BF16)
            rest = (v - top.astype(F32)).astype(BF16)
            acc = dot(top, band_z[...]) + dot(rest, band_z[...])
            acc = acc + dot(band_y[...], top) + dot(band_y[...], rest)
            acc = acc.reshape(ROWS, ny, nz)
            total = jnp.zeros((8, nz), F32)
            for i in range(ROWS):
                x = x0 + i
                centre = own[cur, s, x]
                value = acc[i] + sources[t, s, x] + CENTRE * centre
                for k in range(1, HALO + 1):
                    near = [own[cur, s, y] for y in (x + k, x - k) if 0 <= y < slab]
                    pair = near[0] + near[1] if len(near) == 2 else near[0]
                    value = value + REACH[k] * pair
                fresh = 2.0 * centre - own[nxt, s, x] + vel[x] * value
                own[nxt, s, x] = fresh
                if inner:
                    total = total + record(t, s, x, fresh)
            if inner:
                if b == 1:
                    squares[t, s] = total
                else:
                    squares[t, s] = squares[t, s] + total

    def edge_stage(t, s):
        cur = lax.rem(t, 2)
        nxt = 1 - cur
        for side in range(2):

            @pl.when(has[side])
            def _():
                halo_copy(t, s, 1 - side).wait_recv()

            for i in range(HALO):
                x = i if side == 0 else slab - 1 - i
                add = None
                for k in range(i + 1, HALO + 1):
                    far = k - i - 1
                    plane = halo[cur, s, side, HALO - 1 - far if side == 0 else far]
                    term = REACH[k] * plane
                    add = term if add is None else add + term
                own[nxt, s, x] = own[nxt, s, x] + vel[x] * add

            @pl.when(has[side] & (t < steps - 1))
            def _():
                halo_copy(t + 1, s, side).start()

        for side in range(2):

            @pl.when(has[side])
            def _():
                halo_copy(t, s, side).wait_send()

        total = squares[t, s]
        for i in range(HALO):
            for x in (i, slab - 1 - i):
                total = total + record(t, s, x, own[nxt, s, x])
        squares[t, s] = total

        @pl.when(t == steps - 2)
        def _():
            before_copy(s).start()

        @pl.when(t == steps - 1)
        def _():
            last_copy(s).start()

    def before_copy(s):
        return pltpu.make_async_copy(
            own.at[(steps - 1) % 2, s], before_hbm.at[s], out_before.at[s]
        )

    def last_copy(s):
        return pltpu.make_async_copy(own.at[steps % 2, s], last_hbm.at[s], out_last.at[s])

    rounds = 0
    while 2 ** (rounds + 1) < n // 2:
        rounds += 1
    rounds += 1

    def meet(m):
        for j in range(rounds + 1):

            @pl.when(m == shots + 1 + j)
            def _():
                if j > 0:
                    pl.semaphore_wait(ready_sem.at[j - 1], 2)
                if j < rounds:
                    for other in (lax.rem(me + 2**j, n), lax.rem(me + n - 2**j, n)):
                        pl.semaphore_signal(
                            ready_sem.at[j], inc=1, device_id={"gx": other}, device_id_type=MESH
                        )

    def turn(m, carry):
        s = lax.rem(m, shots)
        t = m // shots

        @pl.when(t > 0)
        def _():
            edge_stage(t - 1, s)

        @pl.when(t == 0)
        def _():
            mid_load(s).wait()
            prev_load(s).wait()
            snap_load(s).wait()

        @pl.when(t < steps)
        def _():
            sources_load(t, s).wait()
            block_stage(t, s)

        meet(m)
        return carry

    lax.fori_loop(0, shots * (steps + 1), turn, 0)

    lane = lax.broadcasted_iota(jnp.int32, (1, 128), 1)
    mine = jnp.zeros((1, 128), F32)
    for t in range(steps):
        for s in range(shots):
            amount = jnp.sum(jnp.sum(squares[t, s], axis=0, keepdims=True), axis=1, keepdims=True)
            mine = jnp.where(lane == t * shots + s, amount, mine)
    row_mine[...] = mine
    partner = me + 1 - 2 * lax.rem(me, 2)
    pair = pltpu.make_async_remote_copy(
        src_ref=row_mine,
        dst_ref=row_partner,
        send_sem=pair_send,
        recv_sem=pair_recv,
        device_id={"gx": partner},
        device_id_type=MESH,
    )
    pair.start()
    pair.wait()
    chips = n // 2
    chip = me // 2
    both = mine + row_partner[...]
    row_chip[...] = both
    rows_all[chip] = both

    def share(k):
        return pltpu.make_async_remote_copy(
            src_ref=row_chip,
            dst_ref=rows_all.at[chip],
            send_sem=all_send,
            recv_sem=all_recv,
            device_id={"gx": lax.rem(me + 2 * k, n)},
            device_id_type=MESH,
        )

    for k in range(1, chips):
        share(k).start()
    everyone = pltpu.make_async_remote_copy(
        src_ref=rows_all.at[pl.ds(0, chips - 1)],
        dst_ref=rows_all.at[pl.ds(0, chips - 1)],
        send_sem=all_send,
        recv_sem=all_recv,
        device_id={"gx": right},
        device_id_type=MESH,
    )
    everyone.wait()
    energy = jnp.sum(rows_all[...], axis=0)
    cells = float(slab * ny * nz) * n
    weight = 1.0 / jnp.sqrt(energy / cells + 1e-6)
    for i in range(steps * shots):
        spread[i] = jnp.broadcast_to(weight[:, i : i + 1], (8, 128))
    def paint(x, carry):
        for y in range(0, ny, 8):
            for z in range(0, nz, 128):
                total = None
                for t in range(steps):
                    for s in range(shots):
                        part = corr[t, s, x, y : y + 8, z : z + 128] * spread[t * shots + s]
                        total = part if total is None else total + part
                image[x, y : y + 8, z : z + 128] = total
        image_copy(x).start()
        return carry

    def image_copy(x):
        return pltpu.make_async_copy(image.at[x], image_hbm.at[x], out_image.at[x])

    lax.fori_loop(0, slab, paint, 0)
    for t in range(steps):
        energy_out[t : t + 1, :] = energy[:, t * shots : (t + 1) * shots]
    for s in range(shots):
        before_copy(s).wait()
        last_copy(s).wait()
    for x in range(slab):
        image_copy(x).wait()


def gather_sources(
    traces_hbm,
    x_hbm,
    y_hbm,
    z_hbm,
    shot_hbm,
    out,
    dense,
    blank,
    traces,
    recv_x,
    recv_y,
    recv_z,
    recv_shot,
    found,
    load_sem,
    blank_sem,
    tile_sem,
):
    steps, shots, slab, ny, nz = out.shape
    count = traces.shape[1]
    pairs = (
        (x_hbm, recv_x),
        (traces_hbm, traces),
        (y_hbm, recv_y),
        (z_hbm, recv_z),
        (shot_hbm, recv_shot),
    )
    loads = [pltpu.make_async_copy(a, b, load_sem.at[i]) for i, (a, b) in enumerate(pairs)]
    for load in loads:
        load.start()
    start = lax.axis_index("gx") * slab
    zeros = jnp.zeros((ny, nz), F32)

    def clear_blank(x, carry):
        blank[x] = zeros
        return carry

    lax.fori_loop(0, slab, clear_blank, 0)

    def blank_copy(t, s):
        return pltpu.make_async_copy(blank, out.at[t, s], blank_sem.at[t, s])

    for t in range(steps):
        for s in range(shots):
            blank_copy(t, s).start()

    def clear(x, carry):
        for t in range(steps):
            for s in range(shots):
                dense[t, s, x] = zeros
        return carry

    lax.fori_loop(0, slab, clear, 0)
    for load in loads:
        load.wait()

    group = 16

    def scan(i, total):
        for j in range(group):
            r = i * group + j
            local = recv_x[r] - start
            found[total] = r
            inside = (local >= 0) & (local < slab)
            total = total + inside.astype(jnp.int32)
        return total

    total = lax.fori_loop(0, count // group, scan, 0)
    lane = lax.broadcasted_iota(jnp.int32, (1, nz), 1)

    def add(i, carry):
        r = found[i]
        s, x, y = recv_shot[r], recv_x[r] - start, recv_y[r]
        here = lane == recv_z[r]
        for t in range(steps):
            row = dense[t, s, x, pl.ds(y, 1), :]
            dense[t, s, x, pl.ds(y, 1), :] = row + jnp.where(here, traces[t, r] * SCALE, 0.0)
        return carry

    lax.fori_loop(0, total, add, 0)
    for t in range(steps):
        for s in range(shots):
            blank_copy(t, s).wait()

    def tile_copy(i, t):
        r = found[i]
        s, x = recv_shot[r], recv_x[r] - start
        rows = pl.ds(pl.multiple_of((recv_y[r] // 8) * 8, 8), 8)
        return pltpu.make_async_copy(
            dense.at[t, s, x, rows], out.at[t, s, x, rows], tile_sem.at[lax.rem(i, FLIGHT), t]
        )

    def chunk(c, carry):
        first = c * FLIGHT
        last = jnp.minimum(first + FLIGHT, total)

        def begin(i, carry):
            for t in range(steps):
                tile_copy(i, t).start()
            return carry

        def finish(i, carry):
            for t in range(steps):
                tile_copy(i, t).wait()
            return carry

        lax.fori_loop(first, last, begin, 0)
        lax.fori_loop(first, last, finish, 0)
        return carry

    lax.fori_loop(0, (total + FLIGHT - 1) // FLIGHT, chunk, 0)


def per_device(
    n, now, prev, velocity, snapshots, traces, recv_x, recv_y, recv_z, recv_shot, snap_step
):
    shots, slab, ny, nz = now.shape
    snaps = snapshots.shape[1]
    steps, count = traces.shape
    hbm = pl.BlockSpec(memory_space=pltpu.HBM)
    vmem = pl.BlockSpec(memory_space=pltpu.VMEM)
    smem = pl.BlockSpec(memory_space=pltpu.SMEM)
    dma = pltpu.SemaphoreType.DMA
    shape = functools.partial(jax.ShapeDtypeStruct, dtype=F32)
    ints = pltpu.SMEM((count,), jnp.int32)
    sources = pl.pallas_call(
        gather_sources,
        out_shape=shape((steps, shots, slab, ny, nz)),
        in_specs=[hbm] * 5,
        out_specs=hbm,
        scratch_shapes=[
            pltpu.VMEM((steps, shots, slab, ny, nz), F32),
            pltpu.VMEM((slab, ny, nz), F32),
            pltpu.SMEM((steps, count), F32),
            ints,
            ints,
            ints,
            ints,
            pltpu.SMEM((count + 1,), jnp.int32),
            dma((5,)),
            dma((steps, shots)),
            dma((FLIGHT, steps)),
        ],
        compiler_params=pltpu.CompilerParams(vmem_limit_bytes=VMEM_SOURCES),
        name="sources",
    )(traces, recv_x, recv_y, recv_z, recv_shot)
    return pl.pallas_call(
        functools.partial(kernel, n),
        out_shape=(
            shape((slab, ny, nz)),
            shape((shots, slab, ny, nz)),
            shape((shots, slab, ny, nz)),
            shape((steps, shots)),
        ),
        in_specs=[hbm] * 5 + [smem],
        out_specs=(hbm, hbm, hbm, vmem),
        scratch_shapes=[
            pltpu.VMEM((2, shots, slab, ny, nz), F32),
            pltpu.VMEM((slab, ny, nz), F32),
            pltpu.VMEM((2, shots, 2, HALO, ny, nz), F32),
            pltpu.VMEM((slab, ny, nz), F32),
            pltpu.VMEM((shots, snaps, slab, ny, nz), F32),
            pltpu.VMEM((steps, shots, slab, ny, nz), F32),
            pltpu.VMEM((steps, shots, slab, ny, nz), F32),
            pltpu.VMEM((ROWS * ny, ROWS * ny), BF16),
            pltpu.VMEM((nz, nz), BF16),
            pltpu.VMEM((steps, shots, 8, nz), F32),
            pltpu.VMEM((steps * shots, 8, 128), F32),
            pltpu.VMEM((1, 128), F32),
            pltpu.VMEM((1, 128), F32),
            pltpu.VMEM((1, 128), F32),
            pltpu.VMEM((n // 2, 1, 128), F32),
            dma((2, shots)),
            dma((shots,)),
            dma((shots,)),
            dma,
            dma((shots,)),
            dma((steps, shots)),
            dma((2, steps, shots)),
            dma((2, steps, shots)),
            pltpu.SemaphoreType.REGULAR((8,)),
            dma,
            dma,
            dma,
            dma,
            dma((shots,)),
            dma((shots,)),
            dma((slab,)),
        ],
        compiler_params=pltpu.CompilerParams(
            collective_id=0, has_side_effects=True, vmem_limit_bytes=VMEM_STEPS
        ),
        name="rtm",
    )(now, prev, velocity, snapshots, sources, snap_step)


def solution(mesh):
    placed = (
        P("grp", "gx", None, None),
        P("grp", "gx", None, None),
        P(("grp", "gx"), None, None),
        P("grp", None, "gx", None, None),
        P("grp", None),
        P("grp"),
        P("grp"),
        P("grp"),
        P("grp"),
        P("grp", None),
    )
    return jax.shard_map(
        functools.partial(per_device, mesh.shape["gx"]),
        mesh=mesh,
        in_specs=placed,
        out_specs=(
            P(("grp", "gx"), None, None),
            P("grp", "gx", None, None),
            P("grp", "gx", None, None),
            P("grp", None),
        ),
        check_vma=False,
    )
```
